32 devices in a mesh: row: 8 (over y, x, core), col: 4 (over z).
Axes of the slice: x: 2, y: 2, z: 4, core: 2. Of those that a mesh axis runs over, the one named last changes fastest.
Arguments:
- tiles: bfloat16 [16384, 128, 128], P(('row', 'col'))
- row_tiles: int32 [16384], P(('row', 'col')), may hold values from 0 to 127, as said below
- col_tiles: int32 [16384], P(('row', 'col')), may hold values from 0 to 1023, as said below
- counts: int32 [32], P(('row', 'col')), may hold values from 128 to 512, as said below
- right_basis: float32 [100, 131072], P(None, ('row', 'col'))
- left_basis: float32 [100, 131072], P(None, ('row', 'col'))
- start: float32 [131072], P(('row', 'col'))
Outputs:
- left_vectors: float32 [2, 131072], P(None, ('row', 'col'))
- right_vectors: float32 [2, 131072], P(None, ('row', 'col'))
- coefficients: float32 [5], replicated
The draws below stay inside these ranges and needn't reach their ends.
Inputs may be any that keep to these rules, and one draw needn't show every extreme that they name: `row_tiles`: tile rows lie within a row group. `col_tiles`: device d owns tile columns d * 32 up to (d + 1) * 32 - 1. The 512 slots of one device name at most 8 distinct tile columns owned by any one device; in every draw some owner receives exactly 8 distinct live tile columns from every device. `counts`: slots at or beyond a block's count hold no part of the matrix; in every draw some block has 512 live slots.
All inputs are finite; a program needn't handle non-finite values.
Results may differ from the reference program's by a relative error of at most 0.0045.
The reference program's roundings to bfloat16 on the way count: a program that leaves them out, or rounds other values in their place, can miss the bound.
Values may be sent and summed in bfloat16 or wider, within the bound.
A program may use at most 128 MiB of HBM per device.

```python
import jax
import jax.numpy as jnp
from jax import lax

ROWS_DEV = 4096
TPD = 512
TILE = 128
K = 100
PEER_TILES = 8
ROWS = 131072
NTILES = 1024
GROUP_TILES = 128
TILES_ALL = 16384
N_ROW = 8
N_COL = 4


def layout(key):
    base = jax.random.fold_in(key, 11)
    devices = TILES_ALL // TPD
    per_owner = ROWS_DEV // TILE
    first_ids = jax.random.randint(jax.random.fold_in(base, 1), (TILES_ALL,), 0, GROUP_TILES)
    second_ids = jax.random.randint(jax.random.fold_in(base, 2), (TILES_ALL,), 0, GROUP_TILES)
    row_ids = jnp.minimum(first_ids, second_ids).astype(jnp.int32)
    owners = jax.random.randint(jax.random.fold_in(base, 3), (TILES_ALL,), 0, devices)
    picks = jax.random.randint(jax.random.fold_in(base, 4), (TILES_ALL,), 0, PEER_TILES)
    scores = jax.random.randint(jax.random.fold_in(base, 5), (devices, devices, per_owner), 0, 1048576) * per_owner + jnp.arange(per_owner, dtype=jnp.int32)
    ranked = jnp.argsort(scores, axis=-1)[:, :, :PEER_TILES].astype(jnp.int32)
    special_owner = jax.random.randint(jax.random.fold_in(base, 6), (), 0, devices)
    slot_place = jnp.arange(TILES_ALL, dtype=jnp.int32) % TPD
    leading = slot_place < PEER_TILES
    owners = jnp.where(leading, special_owner, owners)
    picks = jnp.where(leading, slot_place, picks)
    sender = jnp.arange(TILES_ALL, dtype=jnp.int32) // TPD
    col_ids = (owners * per_owner + ranked[sender, owners, picks]).astype(jnp.int32)
    levels = jax.random.randint(jax.random.fold_in(base, 7), (devices,), 0, 8)
    counts = jnp.where(levels < 3, TPD, jnp.where(levels < 6, TPD // 2, TPD // 4))
    chosen = jax.random.randint(jax.random.fold_in(base, 8), (), 0, devices)
    counts = jnp.where(jnp.arange(devices) == chosen, TPD, counts).astype(jnp.int32)
    return (row_ids, col_ids, counts)


def tile_values(key):
    return jax.random.normal(jax.random.fold_in(key, 12), (TILES_ALL, TILE, TILE), jnp.float32) * (0.35 / TILE ** 0.5)


def noises(key):
    first_key = jax.random.fold_in(key, 14)
    second_key = jax.random.fold_in(key, 15)
    return (jax.random.normal(first_key, (ROWS,), jnp.float32), jax.random.normal(second_key, (ROWS,), jnp.float32))


def right_values(key):
    own_part = jax.random.normal(jax.random.fold_in(key, 13), (K, ROWS), jnp.float32)
    shared_part = jax.random.normal(jax.random.fold_in(key, 18), (ROWS,), jnp.float32)
    return own_part + 0.1 * shared_part[None, :]


def apply_rows(key, vector):
    devices = TILES_ALL // TPD
    col_count = GROUP_TILES * TILE // ROWS_DEV
    row_ids, col_ids, counts = layout(key)
    table = vector.reshape(NTILES, TILE)
    slots = jnp.arange(TPD)
    members = (tile_values(key).reshape(devices, TPD, TILE, TILE), row_ids.reshape(devices, TPD), col_ids.reshape(devices, TPD), counts, jnp.arange(devices))

    def advance(running, member):
        blocks, rows_here, cols_here, count, device = member
        weights = (slots < count).astype(jnp.float32)
        products = jnp.einsum('tij,tj->ti', blocks, table[cols_here]) * weights[:, None]
        target = device // col_count * GROUP_TILES + rows_here
        return (running + jax.ops.segment_sum(products, target, num_segments=NTILES), None)
    return lax.scan(advance, jnp.zeros((NTILES, TILE), jnp.float32), members)[0].reshape(-1)


def draw_tiles(key, part):
    return tile_values(key).astype(jnp.bfloat16)


def draw_row_tiles(key, part):
    return layout(key)[0]


def draw_col_tiles(key, part):
    return layout(key)[1]


def draw_counts(key, part):
    return layout(key)[2]


def draw_right_basis(key, part):
    return right_values(key)


def draw_left_basis(key, part):
    first_noise = noises(key)[0]
    image = apply_rows(key, first_noise)
    image = image / jnp.sqrt(jnp.mean(image * image) + 1e-06)
    own_part = jax.random.normal(jax.random.fold_in(key, 16), (K, ROWS), jnp.float32)
    shared_part = jax.random.normal(jax.random.fold_in(key, 19), (ROWS,), jnp.float32)
    others = own_part + 0.1 * shared_part[None, :]
    return others.at[0].set(image)


def draw_start(key, part):
    first_noise, second_noise = noises(key)
    raw_mix = jax.random.normal(jax.random.fold_in(key, 17), (K,), jnp.float32)
    mixing = (raw_mix - jnp.mean(raw_mix)) * (1.2 / K ** 0.5) + 2.5 / K
    return first_noise + second_noise + jnp.dot(mixing, right_values(key))


def setup_inputs(seed: int = 0) -> dict:
    key_list = jax.random.split(jax.random.key(seed), 8)
    return {
        "tiles": draw_tiles(jax.random.fold_in(key_list[7], 71), 0),
        "row_tiles": draw_row_tiles(jax.random.fold_in(key_list[7], 71), 0),
        "col_tiles": draw_col_tiles(jax.random.fold_in(key_list[7], 71), 0),
        "counts": draw_counts(jax.random.fold_in(key_list[7], 71), 0),
        "right_basis": draw_right_basis(jax.random.fold_in(key_list[7], 71), 0),
        "left_basis": draw_left_basis(jax.random.fold_in(key_list[7], 71), 0),
        "start": draw_start(jax.random.fold_in(key_list[7], 71), 0),
    }


HIGH = lax.Precision.HIGHEST

def sparse_rows(tiles, row_tiles, col_tiles, counts, vector):
    devices = N_ROW * N_COL
    table = vector.astype(jnp.float32).reshape(NTILES, TILE)
    slots = jnp.arange(TPD, dtype=jnp.int32)
    members = (tiles.reshape(devices, TPD, TILE, TILE), row_tiles.reshape(devices, TPD), col_tiles.reshape(devices, TPD), counts, jnp.arange(devices, dtype=jnp.int32))

    def advance(running, member):
        blocks, rows_here, cols_here, count, device = member
        weights = (slots < count).astype(jnp.float32)
        products = jnp.einsum('tij,tj->ti', blocks.astype(jnp.float32), table[cols_here], precision=HIGH) * weights[:, None]
        target = (device // N_COL * GROUP_TILES + rows_here).astype(jnp.int32)
        return (running + jax.ops.segment_sum(products, target, num_segments=NTILES), None)
    summed = lax.scan(advance, jnp.zeros((NTILES, TILE), jnp.float32), members)[0]
    return summed.reshape(-1)

def sparse_columns(tiles, row_tiles, col_tiles, counts, vector):
    devices = N_ROW * N_COL
    table = vector.astype(jnp.float32).reshape(NTILES, TILE)
    slots = jnp.arange(TPD, dtype=jnp.int32)
    members = (tiles.reshape(devices, TPD, TILE, TILE), row_tiles.reshape(devices, TPD), col_tiles.reshape(devices, TPD), counts, jnp.arange(devices, dtype=jnp.int32))

    def advance(running, member):
        blocks, rows_here, cols_here, count, device = member
        weights = (slots < count).astype(jnp.float32)
        source = (device // N_COL * GROUP_TILES + rows_here).astype(jnp.int32)
        products = jnp.einsum('tij,ti->tj', blocks.astype(jnp.float32), table[source], precision=HIGH) * weights[:, None]
        return (running + jax.ops.segment_sum(products, cols_here, num_segments=NTILES), None)
    summed = lax.scan(advance, jnp.zeros((NTILES, TILE), jnp.float32), members)[0]
    return summed.reshape(-1)

def orthogonalize(vector, basis):
    coeffs = jnp.dot(basis, vector, precision=HIGH) / ROWS
    remainder = vector - jnp.dot(coeffs, basis, precision=HIGH)
    norm_value = jnp.sqrt(jnp.sum(remainder * remainder) / ROWS + 1e-06)
    return (remainder / norm_value, norm_value)

def reference(tiles, row_tiles, col_tiles, counts, right_basis, left_basis, start):
    right_one, beta_zero = orthogonalize(start, right_basis)
    image = sparse_rows(tiles, row_tiles, col_tiles, counts, right_one.astype(jnp.bfloat16))
    left_one, alpha_one = orthogonalize(image, left_basis)
    back = sparse_columns(tiles, row_tiles, col_tiles, counts, left_one.astype(jnp.bfloat16)) - alpha_one * right_one
    right_two, beta_one = orthogonalize(back, right_basis)
    image = sparse_rows(tiles, row_tiles, col_tiles, counts, right_two.astype(jnp.bfloat16)) - beta_one * left_one
    left_two, alpha_two = orthogonalize(image, left_basis)
    back = sparse_columns(tiles, row_tiles, col_tiles, counts, left_two.astype(jnp.bfloat16)) - alpha_two * right_two
    right_three, beta_two = orthogonalize(back, right_basis)
    return (jnp.stack([left_one, left_two]), jnp.stack([right_two, right_three]), jnp.stack([beta_zero, alpha_one, beta_one, alpha_two, beta_two]))
```

```python
import functools

import jax
import jax.numpy as jnp
from jax import lax
from jax.experimental import pallas as pl
from jax.experimental.pallas import tpu as pltpu
from jax.sharding import PartitionSpec as P

PEER_TILES = 8
GROUP = 16
UNROLL = 32
CHUNKS = 8
EARLY = 2
MESH = pl.DeviceIdType.MESH
F32 = jnp.float32
BF16 = jnp.bfloat16


def hot(condition):
    return jnp.where(condition, 1.0, 0.0).astype(BF16)


def dot(left, right):
    return jnp.dot(left, right, preferred_element_type=F32)


def exact_dot(selector, values):
    high = values.astype(BF16)
    rest = values - high.astype(F32)
    middle = rest.astype(BF16)
    low = (rest - middle.astype(F32)).astype(BF16)
    return dot(selector, high) + (dot(selector, middle) + dot(selector, low))


def kernel(
    n_row, n_col, row_total,
    tiles_hbm, rows_hbm, cols_hbm, counts_hbm, right_hbm, left_hbm, start_hbm,
    lefts_ref, rights_ref, coeffs_ref,
    tiles, flipped, left_ref, right_ref, row_line, col_line, counts_ref, start_ref,
    place_out, place_buf, c_buf, n_buf, pack_first, x_first, pack, xbuf, outgoing, abuf,
    ypart, rsbuf, share, agbuf, halves, gram_out, gram_in, gram_all,
    r_ref, right_one, left_one, acc_ref, x_gathered, products,
    tile_sems, input_sems, send_sems, recv_sems,
):
    devices = n_row * n_col
    my_row = lax.axis_index("row")
    my_col = lax.axis_index("col")
    me = my_row * n_col + my_col
    slots, size = tiles.shape[0], tiles.shape[1]
    per_owner = start_ref.shape[0]
    group_tiles = per_owner * n_col
    table = devices * PEER_TILES
    basis_rows = right_ref.shape[0]
    gram_rows = gram_out.shape[1]

    barrier = pltpu.get_barrier_semaphore()

    if n_col == 4:
        across = lax.rem(my_col + 2, n_col)
        other_cols = [n_col - 1 - my_col, across, n_col - 1 - across]
    else:
        other_cols = [lax.rem(my_col + i, n_col) for i in range(1, n_col)]

    def each_peer(act):
        for col in other_cols:
            def step(i, _, col=col):
                act(lax.rem(my_row + i, n_row), col)
                return 0

            lax.fori_loop(0, n_row, step, 0)

        def own_step(i, _):
            act(lax.rem(my_row + i, n_row), my_col)
            return 0

        lax.fori_loop(1, n_row, own_step, 0)

    each_peer(
        lambda row, col: pl.semaphore_signal(
            barrier, inc=1, device_id={"row": row, "col": col}, device_id_type=MESH
        )
    )

    small = [(start_hbm, start_ref), (rows_hbm, row_line), (cols_hbm, col_line), (counts_hbm, counts_ref)]
    small_copies = [
        pltpu.make_async_copy(source, target, input_sems.at[i])
        for i, (source, target) in enumerate(small)
    ]
    right_copy = pltpu.make_async_copy(right_hbm, right_ref, input_sems.at[len(small)])
    left_copy = pltpu.make_async_copy(left_hbm, left_ref, input_sems.at[len(small) + 1])
    chunk = slots // CHUNKS
    tile_copies = [
        pltpu.make_async_copy(
            tiles_hbm.at[pl.ds(i * chunk, chunk)], tiles.at[pl.ds(i * chunk, chunk)], tile_sems.at[i]
        )
        for i in range(CHUNKS)
    ]
    for copy in small_copies + [right_copy, left_copy] + tile_copies:
        copy.start()

    phases = [0]

    def next_phase():
        phases[0] += 1
        return phases[0] - 1

    pending = []

    def send_all(source, buf):
        phase = next_phase()

        def send(row, col):
            pltpu.make_async_remote_copy(
                src_ref=source(row * n_col + col), dst_ref=buf.at[me],
                send_sem=send_sems.at[phase], recv_sem=recv_sems.at[phase],
                device_id={"row": row, "col": col}, device_id_type=MESH,
            ).start()

        each_peer(send)
        many = buf.at[pl.ds(0, devices - 1)]
        pending.append((many, phase))
        return lambda: pltpu.make_async_copy(many, many, recv_sems.at[phase]).wait()

    def send_col(source, buf):
        phase = next_phase()
        for col in other_cols:
            pltpu.make_async_remote_copy(
                src_ref=source(col), dst_ref=buf.at[my_col],
                send_sem=send_sems.at[phase], recv_sem=recv_sems.at[phase],
                device_id={"row": my_row, "col": col}, device_id_type=MESH,
            ).start()
        many = buf.at[pl.ds(0, n_col - 1)]
        pending.append((many, phase))
        return lambda: pltpu.make_async_copy(many, many, recv_sems.at[phase]).wait()

    def partial_coeffs(basis, x_ref, buf):
        total = jnp.zeros((basis_rows, size), F32)
        for k in range(per_owner):
            total = total + basis[:, k * size:(k + 1) * size] * x_ref[k:k + 1, :]
        value = x_ref[...]
        acc_ref[0:basis_rows, :] = total
        acc_ref[basis_rows:basis_rows + 1, :] = jnp.sum(value * value, axis=0, keepdims=True)
        buf[me] = jnp.sum(acc_ref[...].T, axis=0, keepdims=True)

    def remainder(basis, x_ref, out_ref, line):
        column = jnp.broadcast_to(line / row_total, (size, size)).T
        for k in range(per_owner):
            part = jnp.sum(
                basis[:, k * size:(k + 1) * size] * column[0:basis_rows, :], axis=0, keepdims=True
            )
            out_ref[k:k + 1, :] = x_ref[k:k + 1, :] - part
        return column

    def gram_norm(line, column, which):
        blocks = size // gram_rows
        gram = jnp.concatenate(
            [gram_all[which * blocks + i] for i in range(blocks)], axis=0
        )
        weighted = jnp.sum(gram * column, axis=0, keepdims=True)
        lane = lax.broadcasted_iota(jnp.int32, (1, size), 1)
        terms = jnp.where(
            lane < basis_rows,
            line / row_total * (weighted - 2.0 * line),
            jnp.where(lane == basis_rows, line, 0.0),
        )
        total = jnp.maximum(jnp.sum(terms, axis=1, keepdims=True), 0.0)
        return jnp.sqrt(total / row_total + 1e-06)

    def put_coeff(i, value):
        coeffs_ref[i:i + 1, :] = jnp.broadcast_to(value, (1, size))

    def put_rows(ref, row, value):
        for k in range(per_owner):
            ref[row:row + 1, k * size:(k + 1) * size] = value[k:k + 1, :]

    def local_gram(basis, which):
        step = 4 * size

        def split(i, _):
            lanes = pl.ds(pl.multiple_of(i * step, step), step)
            value = basis[:, lanes]
            high = value.astype(BF16)
            halves[0:basis_rows, lanes] = high
            halves[size:size + basis_rows, lanes] = (value - high.astype(F32)).astype(BF16)
            return 0

        lax.fori_loop(0, basis.shape[1] // step, split, 0)
        both = lax.dot_general(
            halves[...], halves[...], (((1,), (1,)), ((), ())), preferred_element_type=F32
        )
        top, bottom = both[0:size, :], both[size:2 * size, :]
        gram = top[:, 0:size] + (
            (top[:, size:2 * size] + bottom[:, 0:size]) + bottom[:, size:2 * size]
        )
        blocks = size // gram_rows
        for i in range(blocks):
            gram_out[which * blocks + i] = gram[i * gram_rows:(i + 1) * gram_rows, :]

    def flip(part):
        tile_copies[part].wait()

        def step(i, _):
            first = part * chunk + i * 8
            for h in range(8):
                flipped[first + h] = tiles[first + h].T
            return 0

        lax.fori_loop(0, chunk // 8, step, 0)

    acc_ref[...] = jnp.zeros_like(acc_ref)
    for copy in small_copies + [right_copy]:
        copy.wait()
    partial_coeffs(right_ref, start_ref, c_buf.at[0])

    def upright(line):
        return jnp.broadcast_to(line.astype(F32), (size, slots)).T

    live_line = jnp.where(
        lax.broadcasted_iota(jnp.int32, (1, slots), 1) < counts_ref[0], row_line[...], -1
    )
    live_column = upright(live_line)[:, 0:1]
    columns = upright(col_line[...])[:, 0:1].astype(jnp.int32)
    owner = lax.div(columns, per_owner)
    place = lax.rem(columns, per_owner)
    owner_hot = hot(owner == lax.broadcasted_iota(jnp.int32, (slots, devices), 1))
    place_here = place == lax.broadcasted_iota(jnp.int32, (slots, size), 1)
    named = lax.dot_general(
        owner_hot, hot(place_here), (((0,), (0,)), ((), ())), preferred_element_type=F32
    )
    touched = named > 0.5
    earlier = hot(
        lax.broadcasted_iota(jnp.int32, (size, size), 0)
        <= lax.broadcasted_iota(jnp.int32, (size, size), 1)
    )
    rank = jnp.where(touched, dot(hot(touched), earlier) - 1.0, -1.0)
    for i in range(devices):
        place_out[i] = rank[i:i + 1, :]
    place_buf[me] = place_out[me]

    pl.semaphore_wait(barrier, devices - 1)
    coeffs_in = send_all(lambda target: c_buf.at[0, me], c_buf.at[0])
    places_in = send_all(lambda target: place_out.at[target], place_buf)

    slot_rank = jnp.sum(
        jnp.where(place_here, dot(owner_hot, rank.astype(BF16)), 0.0), axis=1, keepdims=True
    )
    entry = owner.astype(F32) * PEER_TILES + slot_rank
    entry_hot = hot(entry == lax.broadcasted_iota(jnp.int32, (slots, table), 1).astype(F32))
    entry_line = jnp.broadcast_to(entry, (slots, size)).T[0:1, :]
    entry_hot_t = hot(entry_line == lax.broadcasted_iota(jnp.int32, (table, slots), 0).astype(F32))
    row_hot = hot(
        live_column == lax.broadcasted_iota(jnp.int32, (slots, group_tiles), 1).astype(F32)
    )
    row_hot_t = hot(live_line == lax.broadcasted_iota(jnp.int32, (group_tiles, slots), 0))

    halves[...] = jnp.zeros_like(halves)
    local_gram(right_ref, 0)
    left_copy.wait()
    local_gram(left_ref, 1)
    gram_parts_in = send_all(lambda target: gram_out.at[target], gram_in)
    gram_in[me] = gram_out[me]
    for part in range(EARLY):
        flip(part)

    places_in()
    spread = hot(
        lax.div(lax.broadcasted_iota(jnp.int32, (table, devices), 0), PEER_TILES)
        == lax.broadcasted_iota(jnp.int32, (table, devices), 1)
    )
    ranks = jnp.concatenate([place_buf[i] for i in range(devices)], axis=0).astype(BF16)
    wanted = lax.rem(lax.broadcasted_iota(jnp.int32, (table, size), 0), PEER_TILES).astype(F32)
    selector_all = jnp.where(dot(spread, ranks) == wanted, 1.0, 0.0)
    selector = selector_all[:, 0:per_owner].astype(BF16)
    selector_t = selector_all.T[0:per_owner, :].astype(BF16)

    def diagonal(wide):
        index = lax.broadcasted_iota(jnp.int32, (GROUP, size), 0)
        total = wide[:, 0:size]
        for k in range(1, GROUP):
            total = jnp.where(index == k, wide[:, k * size:(k + 1) * size], total)
        return total

    def tile_products(source):
        def one(first):
            vectors = x_gathered[pl.ds(first, GROUP), :]
            block = source[pl.ds(first, GROUP)]
            joined = jnp.concatenate([block[k] for k in range(GROUP)], axis=1)
            return diagonal(dot(vectors, joined))

        def step(g, _):
            firsts = [
                pl.multiple_of(g * (GROUP * UNROLL) + h * GROUP, GROUP) for h in range(UNROLL)
            ]
            found = [one(first) for first in firsts]
            for first, value in zip(firsts, found):
                products[pl.ds(first, GROUP), :] = value
            return 0

        lax.fori_loop(0, slots // (GROUP * UNROLL), step, 0)

    def rows_product(index, values):
        x_gathered[...] = dot(entry_hot, values).astype(BF16)
        tile_products(flipped)
        ypart[index] = exact_dot(row_hot_t, products[...]).reshape(n_col, per_owner, size)
        rows_in = send_col(lambda target: ypart.at[index, target], rsbuf.at[index])
        rsbuf[index, my_col] = ypart[index, my_col]
        rows_in()
        total = rsbuf[index, 0]
        for i in range(1, n_col):
            total = total + rsbuf[index, i]
        return total

    def columns_product(index):
        values = agbuf[index].reshape(group_tiles, size)
        x_gathered[...] = dot(row_hot, values).astype(BF16)
        tile_products(tiles)
        outgoing[index] = exact_dot(entry_hot_t, products[...]).reshape(devices, PEER_TILES, size)
        sums_in = send_all(lambda target: outgoing.at[index, target], abuf.at[index])
        abuf[index, me] = outgoing[index, me]
        sums_in()
        return exact_dot(selector_t, abuf[index].reshape(table, size))

    def orthogonalize(basis, which, x_ref, out_ref, index):
        partial_coeffs(basis, x_ref, c_buf.at[index])
        send_all(lambda target: c_buf.at[index, me], c_buf.at[index])()
        line = jnp.sum(c_buf[index], axis=0)
        column = remainder(basis, x_ref, out_ref, line)
        norm = gram_norm(line, column, which)
        put_coeff(index, norm)
        return norm, out_ref[...] / norm

    scratch = r_ref
    coeffs_in()
    remainder(right_ref, start_ref, scratch.at[1], jnp.sum(c_buf[0], axis=0))
    value = scratch[1]
    n_buf[me] = jnp.sum(value * value, axis=0, keepdims=True)
    norms_in = send_all(lambda target: n_buf.at[me], n_buf)
    pack_first[...] = exact_dot(selector, value).reshape(devices, PEER_TILES, size)
    values_in = send_all(lambda target: pack_first.at[target], x_first)
    x_first[me] = pack_first[me]
    for part in range(EARLY, CHUNKS):
        flip(part)
    gram_parts_in()
    gram_total = gram_in[0]
    for i in range(1, devices):
        gram_total = gram_total + gram_in[i]
    gram_all[me] = gram_total
    norms_in()
    norm = jnp.sqrt(
        jnp.sum(jnp.sum(n_buf[...], axis=0), axis=1, keepdims=True) / row_total + 1e-06
    )
    put_coeff(0, norm)
    right_one[...] = scratch[1] / norm
    values_in()
    gram_in_all = send_all(lambda target: gram_all.at[me], gram_all)

    scratch[0] = rows_product(0, (x_first[...].reshape(table, size) / norm).astype(BF16))
    for index in range(2):
        if index == 0:
            gram_in_all()
        norm, value = orthogonalize(left_ref, 1, scratch.at[0], scratch.at[1], 2 * index + 1)
        share[index] = value.astype(BF16)
        values_in = send_col(lambda target: share.at[index], agbuf.at[index])
        agbuf[index, my_col] = share[index]
        left_one[...] = value
        put_rows(lefts_ref, index, left_one)
        values_in()
        scratch[0] = columns_product(index) - norm * right_one[...]

        norm, value = orthogonalize(right_ref, 0, scratch.at[0], scratch.at[1], 2 * index + 2)
        if index == 0:
            packed = dot(selector, value.astype(BF16)).reshape(devices, PEER_TILES, size)
            pack[...] = packed.astype(BF16)
            values_in = send_all(lambda target: pack.at[target], xbuf)
            xbuf[me] = pack[me]
        right_one[...] = value
        put_rows(rights_ref, index, right_one)
        if index == 0:
            values_in()
            found = xbuf[...].astype(F32).reshape(table, size).astype(BF16)
            scratch[0] = rows_product(1, found) - norm * left_one[...]

    for many, phase in pending:
        pltpu.make_async_copy(many, many, send_sems.at[phase]).wait()


def finish(lefts_in, rights_in, coeffs_in, lefts, rights, line):
    lefts[...] = lefts_in[...]
    rights[...] = rights_in[...]
    for i in range(5):
        line[i] = coeffs_in[i, 0]


def shards(tiles, row_tiles, col_tiles, counts, right_basis, left_basis, start):
    n_row, n_col = lax.axis_size("row"), lax.axis_size("col")
    devices = n_row * n_col
    slots, size = tiles.shape[0], tiles.shape[1]
    rows_dev = start.shape[0]
    per_owner = rows_dev // size
    row_total = float(rows_dev * devices)
    vmem = pl.BlockSpec(memory_space=pltpu.VMEM)
    hbm = pl.BlockSpec(memory_space=pl.ANY)
    n_phases = 17
    gram_rows = 2 * size // devices
    lefts, rights, coeffs = pl.pallas_call(
        functools.partial(kernel, n_row, n_col, row_total),
        out_shape=(
            jax.ShapeDtypeStruct((2, rows_dev), F32),
            jax.ShapeDtypeStruct((2, rows_dev), F32),
            jax.ShapeDtypeStruct((8, size), F32),
        ),
        in_specs=[hbm] * 7,
        out_specs=(vmem, vmem, vmem),
        scratch_shapes=[
            pltpu.VMEM(tiles.shape, BF16),
            pltpu.VMEM(tiles.shape, BF16),
            pltpu.VMEM(left_basis.shape, F32),
            pltpu.VMEM(right_basis.shape, F32),
            pltpu.VMEM((1, slots), jnp.int32),
            pltpu.VMEM((1, slots), jnp.int32),
            pltpu.SMEM((1,), jnp.int32),
            pltpu.VMEM((per_owner, size), F32),
            pltpu.VMEM((devices, 1, size), F32),
            pltpu.VMEM((devices, 1, size), F32),
            pltpu.VMEM((5, devices, 1, size), F32),
            pltpu.VMEM((devices, 1, size), F32),
            pltpu.VMEM((devices, PEER_TILES, size), F32),
            pltpu.VMEM((devices, PEER_TILES, size), F32),
            pltpu.VMEM((devices, PEER_TILES, size), BF16),
            pltpu.VMEM((devices, PEER_TILES, size), BF16),
            pltpu.VMEM((2, devices, PEER_TILES, size), F32),
            pltpu.VMEM((2, devices, PEER_TILES, size), F32),
            pltpu.VMEM((2, n_col, per_owner, size), F32),
            pltpu.VMEM((2, n_col, per_owner, size), F32),
            pltpu.VMEM((2, per_owner, size), BF16),
            pltpu.VMEM((2, n_col, per_owner, size), BF16),
            pltpu.VMEM((2 * size, rows_dev), BF16),
            pltpu.VMEM((devices, gram_rows, size), F32),
            pltpu.VMEM((devices, gram_rows, size), F32),
            pltpu.VMEM((devices, gram_rows, size), F32),
            pltpu.VMEM((2, per_owner, size), F32),
            pltpu.VMEM((per_owner, size), F32),
            pltpu.VMEM((per_owner, size), F32),
            pltpu.VMEM((size, size), F32),
            pltpu.VMEM((slots, size), BF16),
            pltpu.VMEM((slots, size), F32),
            pltpu.SemaphoreType.DMA((CHUNKS,)),
            pltpu.SemaphoreType.DMA((6,)),
            pltpu.SemaphoreType.DMA((n_phases,)),
            pltpu.SemaphoreType.DMA((n_phases,)),
        ],
        compiler_params=pltpu.CompilerParams(
            collective_id=0, has_side_effects=True, vmem_limit_bytes=60 * 1024 * 1024
        ),
    )(
        tiles, row_tiles.reshape(1, slots), col_tiles.reshape(1, slots), counts, right_basis, left_basis, start.reshape(per_owner, size),
    )
    lefts, rights, line = pl.pallas_call(
        finish,
        out_shape=(
            jax.ShapeDtypeStruct(lefts.shape, F32),
            jax.ShapeDtypeStruct(rights.shape, F32),
            jax.ShapeDtypeStruct((5,), F32),
        ),
        in_specs=[vmem, vmem, pl.BlockSpec(memory_space=pltpu.SMEM)],
        out_specs=(vmem, vmem, pl.BlockSpec(memory_space=pltpu.SMEM)),
    )(lefts, rights, coeffs)
    return lefts, rights, line


def solution(mesh):
    placed = (
        P(("row", "col"), None, None),
        P(("row", "col")),
        P(("row", "col")),
        P(("row", "col")),
        P(None, ("row", "col")),
        P(None, ("row", "col")),
        P(("row", "col")),
    )
    return jax.shard_map(
        shards,
        mesh=mesh,
        in_specs=placed,
        out_specs=(P(None, ("row", "col")), P(None, ("row", "col")), P()),
        check_vma=False,
    )
```

```python
import functools

import jax
import jax.numpy as jnp
from jax import lax
from jax.experimental import pallas as pl
from jax.experimental.pallas import tpu as pltpu
from jax.sharding import PartitionSpec as P

PEER_TILES = 8
GROUP = 16
UNROLL = 16
CHUNKS = 16
DEPTH = 4
EARLY = 4
MESH = pl.DeviceIdType.MESH
F32 = jnp.float32
BF16 = jnp.bfloat16


def hot(condition):
    return jnp.where(condition, 1.0, 0.0).astype(BF16)


def dot(left, right):
    return jnp.dot(left, right, preferred_element_type=F32)


def exact_dot(selector, values):
    high = values.astype(BF16)
    rest = values - high.astype(F32)
    middle = rest.astype(BF16)
    low = (rest - middle.astype(F32)).astype(BF16)
    return dot(selector, high) + (dot(selector, middle) + dot(selector, low))


def kernel(
    n_row, n_col, row_total,
    tiles_hbm, rows_hbm, cols_hbm, counts_hbm, right_hbm, left_hbm, start_hbm,
    lefts_ref, rights_ref, coeffs_ref,
    tiles, flipped, left_ref, right_ref, row_line, col_line, counts_ref, start_ref,
    place_out, place_buf, c_buf, n_buf, pack_first, x_first, pack, xbuf, outgoing, abuf,
    ypart, rsbuf, share, agbuf, halves, gram_out, gram_in, gram_all,
    r_ref, right_one, left_one, acc_ref, x_gathered, products,
    tile_sems, input_sems, send_sems, recv_sems,
):
    devices = n_row * n_col
    my_row = lax.axis_index("row")
    my_col = lax.axis_index("col")
    me = my_row * n_col + my_col
    slots, size = tiles.shape[0], tiles.shape[1]
    per_owner = start_ref.shape[0]
    group_tiles = per_owner * n_col
    table = devices * PEER_TILES
    basis_rows = right_ref.shape[0]
    gram_rows = gram_out.shape[2]

    barrier = pltpu.get_barrier_semaphore()

    if n_col == 4:
        across = lax.rem(my_col + 2, n_col)
        other_cols = [n_col - 1 - my_col, across, n_col - 1 - across]
    else:
        other_cols = [lax.rem(my_col + i, n_col) for i in range(1, n_col)]

    def each_peer(act):
        for col in other_cols:
            def step(i, _, col=col):
                act(lax.rem(my_row + i, n_row), col)
                return 0

            lax.fori_loop(0, n_row, step, 0)

        def own_step(i, _):
            act(lax.rem(my_row + i, n_row), my_col)
            return 0

        lax.fori_loop(1, n_row, own_step, 0)

    each_peer(
        lambda row, col: pl.semaphore_signal(
            barrier, inc=1, device_id={"row": row, "col": col}, device_id_type=MESH
        )
    )

    small = [(start_hbm, start_ref), (rows_hbm, row_line), (cols_hbm, col_line), (counts_hbm, counts_ref)]
    small_copies = [
        pltpu.make_async_copy(source, target, input_sems.at[i])
        for i, (source, target) in enumerate(small)
    ]
    right_copy = pltpu.make_async_copy(right_hbm, right_ref, input_sems.at[len(small)])
    left_copy = pltpu.make_async_copy(left_hbm, left_ref, input_sems.at[len(small) + 1])
    chunk = slots // CHUNKS
    tile_copies = [
        pltpu.make_async_copy(
            tiles_hbm.at[pl.ds(i * chunk, chunk)], tiles.at[pl.ds(i * chunk, chunk)], tile_sems.at[i]
        )
        for i in range(CHUNKS)
    ]
    for copy in [right_copy] + small_copies:
        copy.start()

    phases = [0]

    def next_phase():
        phases[0] += 1
        return phases[0] - 1

    pending = []

    def send_all(source, buf):
        phase = next_phase()

        def send(row, col):
            pltpu.make_async_remote_copy(
                src_ref=source(row * n_col + col), dst_ref=buf.at[me],
                send_sem=send_sems.at[phase], recv_sem=recv_sems.at[phase],
                device_id={"row": row, "col": col}, device_id_type=MESH,
            ).start()

        each_peer(send)
        many = buf.at[pl.ds(0, devices - 1)]
        pending.append((many, phase))
        return lambda: pltpu.make_async_copy(many, many, recv_sems.at[phase]).wait()

    def send_col(source, buf):
        phase = next_phase()
        for col in other_cols:
            pltpu.make_async_remote_copy(
                src_ref=source(col), dst_ref=buf.at[my_col],
                send_sem=send_sems.at[phase], recv_sem=recv_sems.at[phase],
                device_id={"row": my_row, "col": col}, device_id_type=MESH,
            ).start()
        many = buf.at[pl.ds(0, n_col - 1)]
        pending.append((many, phase))
        return lambda: pltpu.make_async_copy(many, many, recv_sems.at[phase]).wait()

    def partial_coeffs(basis, x_ref, buf):
        total = jnp.zeros((basis_rows, size), F32)
        for k in range(per_owner):
            total = total + basis[:, k * size:(k + 1) * size] * x_ref[k:k + 1, :]
        value = x_ref[...]
        acc_ref[0:basis_rows, :] = total
        acc_ref[basis_rows:basis_rows + 1, :] = jnp.sum(value * value, axis=0, keepdims=True)
        buf[me] = jnp.sum(acc_ref[...].T, axis=0, keepdims=True)

    def remainder(basis, x_ref, out_ref, line):
        column = jnp.broadcast_to(line / row_total, (size, size)).T
        for k in range(per_owner):
            part = jnp.sum(
                basis[:, k * size:(k + 1) * size] * column[0:basis_rows, :], axis=0, keepdims=True
            )
            out_ref[k:k + 1, :] = x_ref[k:k + 1, :] - part
        return column

    def gram_norm(line, column, which):
        gram = jnp.concatenate([gram_all[which, i] for i in range(devices)], axis=0)
        weighted = jnp.sum(gram * column, axis=0, keepdims=True)
        lane = lax.broadcasted_iota(jnp.int32, (1, size), 1)
        terms = jnp.where(
            lane < basis_rows,
            line / row_total * (weighted - 2.0 * line),
            jnp.where(lane == basis_rows, line, 0.0),
        )
        total = jnp.maximum(jnp.sum(terms, axis=1, keepdims=True), 0.0)
        return jnp.sqrt(total / row_total + 1e-06)

    def put_coeff(i, value):
        coeffs_ref[i:i + 1, :] = jnp.broadcast_to(value, (1, size))

    def put_rows(ref, row, value):
        for k in range(per_owner):
            ref[row:row + 1, k * size:(k + 1) * size] = value[k:k + 1, :]

    def local_gram(basis, which):
        step = 4 * size

        def split(i, _):
            lanes = pl.ds(pl.multiple_of(i * step, step), step)
            value = basis[:, lanes]
            high = value.astype(BF16)
            halves[0:basis_rows, lanes] = high
            halves[size:size + basis_rows, lanes] = (value - high.astype(F32)).astype(BF16)
            return 0

        lax.fori_loop(0, basis.shape[1] // step, split, 0)
        both = lax.dot_general(
            halves[...], halves[...], (((1,), (1,)), ((), ())), preferred_element_type=F32
        )
        top, bottom = both[0:size, :], both[size:2 * size, :]
        gram = top[:, 0:size] + (
            (top[:, size:2 * size] + bottom[:, 0:size]) + bottom[:, size:2 * size]
        )
        for i in range(devices):
            gram_out[which, i] = gram[i * gram_rows:(i + 1) * gram_rows, :]

    def share_gram_parts(which):
        gram_in[which, me] = gram_out[which, me]
        return send_all(lambda target: gram_out.at[which, target], gram_in.at[which])

    def share_gram_sums(which):
        total = gram_in[which, 0]
        for i in range(1, devices):
            total = total + gram_in[which, i]
        gram_all[which, me] = total
        return send_all(lambda target: gram_all.at[which, me], gram_all.at[which])

    def flip(part):
        tile_copies[part].wait()
        if part + DEPTH < CHUNKS:
            tile_copies[part + DEPTH].start()
        first = part * chunk
        found = [tiles[first + h].T for h in range(chunk)]
        for h in range(chunk):
            flipped[first + h] = found[h]

    acc_ref[...] = jnp.zeros_like(acc_ref)
    for copy in small_copies:
        copy.wait()

    def upright(line):
        return jnp.broadcast_to(line.astype(F32), (size, slots)).T

    live_line = jnp.where(
        lax.broadcasted_iota(jnp.int32, (1, slots), 1) < counts_ref[0], row_line[...], -1
    )
    live_column = upright(live_line)[:, 0:1]
    columns = upright(col_line[...])[:, 0:1].astype(jnp.int32)
    owner = lax.div(columns, per_owner)
    place = lax.rem(columns, per_owner)
    owner_hot = hot(owner == lax.broadcasted_iota(jnp.int32, (slots, devices), 1))
    place_here = place == lax.broadcasted_iota(jnp.int32, (slots, size), 1)
    named = lax.dot_general(
        owner_hot, hot(place_here), (((0,), (0,)), ((), ())), preferred_element_type=F32
    )
    touched = named > 0.5
    earlier = hot(
        lax.broadcasted_iota(jnp.int32, (size, size), 0)
        <= lax.broadcasted_iota(jnp.int32, (size, size), 1)
    )
    rank = jnp.where(touched, dot(hot(touched), earlier) - 1.0, -1.0)
    for i in range(devices):
        place_out[i] = rank[i:i + 1, :]
    place_buf[me] = place_out[me]

    right_copy.wait()
    for copy in [left_copy] + tile_copies[0:DEPTH]:
        copy.start()
    partial_coeffs(right_ref, start_ref, c_buf.at[0])
    pl.semaphore_wait(barrier, devices - 1)
    coeffs_in = send_all(lambda target: c_buf.at[0, me], c_buf.at[0])
    places_in = send_all(lambda target: place_out.at[target], place_buf)

    slot_rank = jnp.sum(
        jnp.where(place_here, dot(owner_hot, rank.astype(BF16)), 0.0), axis=1, keepdims=True
    )
    entry = owner.astype(F32) * PEER_TILES + slot_rank
    entry_hot = hot(entry == lax.broadcasted_iota(jnp.int32, (slots, table), 1).astype(F32))
    entry_line = jnp.broadcast_to(entry, (slots, size)).T[0:1, :]
    entry_hot_t = hot(entry_line == lax.broadcasted_iota(jnp.int32, (table, slots), 0).astype(F32))
    row_hot = hot(
        live_column == lax.broadcasted_iota(jnp.int32, (slots, group_tiles), 1).astype(F32)
    )
    row_hot_t = hot(live_line == lax.broadcasted_iota(jnp.int32, (group_tiles, slots), 0))

    halves[...] = jnp.zeros_like(halves)
    left_copy.wait()
    local_gram(left_ref, 1)
    left_gram_in = share_gram_parts(1)
    for part in range(EARLY):
        flip(part)

    places_in()
    spread = hot(
        lax.div(lax.broadcasted_iota(jnp.int32, (table, devices), 0), PEER_TILES)
        == lax.broadcasted_iota(jnp.int32, (table, devices), 1)
    )
    ranks = jnp.concatenate([place_buf[i] for i in range(devices)], axis=0).astype(BF16)
    wanted = lax.rem(lax.broadcasted_iota(jnp.int32, (table, size), 0), PEER_TILES).astype(F32)
    selector_all = jnp.where(dot(spread, ranks) == wanted, 1.0, 0.0)
    selector = selector_all[:, 0:per_owner].astype(BF16)
    selector_t = selector_all.T[0:per_owner, :].astype(BF16)

    def diagonal(wide):
        index = lax.broadcasted_iota(jnp.int32, (GROUP, size), 0)
        total = wide[:, 0:size]
        for k in range(1, GROUP):
            total = jnp.where(index == k, wide[:, k * size:(k + 1) * size], total)
        return total

    def tile_products(source):
        def one(first):
            vectors = x_gathered[pl.ds(first, GROUP), :]
            block = source[pl.ds(first, GROUP)]
            joined = jnp.concatenate([block[k] for k in range(GROUP)], axis=1)
            return diagonal(dot(vectors, joined))

        def step(g, _):
            firsts = [
                pl.multiple_of(g * (GROUP * UNROLL) + h * GROUP, GROUP) for h in range(UNROLL)
            ]
            found = [one(first) for first in firsts]
            for first, value in zip(firsts, found):
                products[pl.ds(first, GROUP), :] = value
            return 0

        lax.fori_loop(0, slots // (GROUP * UNROLL), step, 0)

    def rows_product(index, values, meanwhile=lambda: None):
        x_gathered[...] = dot(entry_hot, values).astype(BF16)
        tile_products(flipped)
        ypart[index] = exact_dot(row_hot_t, products[...]).reshape(n_col, per_owner, size)
        rows_in = send_col(lambda target: ypart.at[index, target], rsbuf.at[index])
        rsbuf[index, my_col] = ypart[index, my_col]
        meanwhile()
        rows_in()
        total = rsbuf[index, 0]
        for i in range(1, n_col):
            total = total + rsbuf[index, i]
        return total

    def columns_product(index):
        values = agbuf[index].reshape(group_tiles, size)
        x_gathered[...] = dot(row_hot, values).astype(BF16)
        tile_products(tiles)
        outgoing[index] = exact_dot(entry_hot_t, products[...]).reshape(devices, PEER_TILES, size)
        sums_in = send_all(lambda target: outgoing.at[index, target], abuf.at[index])
        abuf[index, me] = outgoing[index, me]
        sums_in()
        return exact_dot(selector_t, abuf[index].reshape(table, size))

    def orthogonalize(basis, which, x_ref, out_ref, index, meanwhile=lambda: None):
        partial_coeffs(basis, x_ref, c_buf.at[index])
        coeffs_in = send_all(lambda target: c_buf.at[index, me], c_buf.at[index])
        meanwhile()
        coeffs_in()
        line = jnp.sum(c_buf[index], axis=0)
        column = remainder(basis, x_ref, out_ref, line)
        norm = gram_norm(line, column, which)
        put_coeff(index, norm)
        return norm, out_ref[...] / norm

    scratch = r_ref
    coeffs_in()
    remainder(right_ref, start_ref, scratch.at[1], jnp.sum(c_buf[0], axis=0))
    value = scratch[1]
    n_buf[me] = jnp.sum(value * value, axis=0, keepdims=True)
    norms_in = send_all(lambda target: n_buf.at[me], n_buf)
    pack_first[...] = exact_dot(selector, value).reshape(devices, PEER_TILES, size)
    values_in = send_all(lambda target: pack_first.at[target], x_first)
    x_first[me] = pack_first[me]
    for part in range(EARLY, CHUNKS):
        flip(part)
    left_gram_in()
    left_gram_in = share_gram_sums(1)
    norms_in()
    norm = jnp.sqrt(
        jnp.sum(jnp.sum(n_buf[...], axis=0), axis=1, keepdims=True) / row_total + 1e-06
    )
    put_coeff(0, norm)
    right_one[...] = scratch[1] / norm
    values_in()

    first_values = (x_first[...].reshape(table, size) / norm).astype(BF16)
    scratch[0] = rows_product(0, first_values, lambda: local_gram(right_ref, 0))
    for index in range(2):
        if index == 0:
            left_gram_in()
        waits = []

        def spread_right_gram():
            if index == 0:
                waits.append(share_gram_parts(0))

        norm, value = orthogonalize(
            left_ref, 1, scratch.at[0], scratch.at[1], 2 * index + 1, spread_right_gram
        )
        share[index] = value.astype(BF16)
        values_in = send_col(lambda target: share.at[index], agbuf.at[index])
        agbuf[index, my_col] = share[index]
        left_one[...] = value
        put_rows(lefts_ref, index, left_one)
        if index == 0:
            waits[0]()
            waits.append(share_gram_sums(0))
        values_in()
        scratch[0] = columns_product(index) - norm * right_one[...]

        if index == 0:
            waits[1]()
        norm, value = orthogonalize(right_ref, 0, scratch.at[0], scratch.at[1], 2 * index + 2)
        if index == 0:
            packed = dot(selector, value.astype(BF16)).reshape(devices, PEER_TILES, size)
            pack[...] = packed.astype(BF16)
            values_in = send_all(lambda target: pack.at[target], xbuf)
            xbuf[me] = pack[me]
        right_one[...] = value
        put_rows(rights_ref, index, right_one)
        if index == 0:
            values_in()
            found = xbuf[...].astype(F32).reshape(table, size).astype(BF16)
            scratch[0] = rows_product(1, found) - norm * left_one[...]

    for many, phase in pending:
        pltpu.make_async_copy(many, many, send_sems.at[phase]).wait()


def finish(lefts_in, rights_in, coeffs_in, lefts, rights, line):
    lefts[...] = lefts_in[...]
    rights[...] = rights_in[...]
    for i in range(5):
        line[i] = coeffs_in[i, 0]


def shards(tiles, row_tiles, col_tiles, counts, right_basis, left_basis, start):
    n_row, n_col = lax.axis_size("row"), lax.axis_size("col")
    devices = n_row * n_col
    slots, size = tiles.shape[0], tiles.shape[1]
    rows_dev = start.shape[0]
    per_owner = rows_dev // size
    row_total = float(rows_dev * devices)
    vmem = pl.BlockSpec(memory_space=pltpu.VMEM)
    hbm = pl.BlockSpec(memory_space=pl.ANY)
    n_phases = 19
    gram_rows = size // devices
    lefts, rights, coeffs = pl.pallas_call(
        functools.partial(kernel, n_row, n_col, row_total),
        out_shape=(
            jax.ShapeDtypeStruct((2, rows_dev), F32),
            jax.ShapeDtypeStruct((2, rows_dev), F32),
            jax.ShapeDtypeStruct((8, size), F32),
        ),
        in_specs=[hbm] * 7,
        out_specs=(vmem, vmem, vmem),
        scratch_shapes=[
            pltpu.VMEM(tiles.shape, BF16),
            pltpu.VMEM(tiles.shape, BF16),
            pltpu.VMEM(left_basis.shape, F32),
            pltpu.VMEM(right_basis.shape, F32),
            pltpu.VMEM((1, slots), jnp.int32),
            pltpu.VMEM((1, slots), jnp.int32),
            pltpu.SMEM((1,), jnp.int32),
            pltpu.VMEM((per_owner, size), F32),
            pltpu.VMEM((devices, 1, size), F32),
            pltpu.VMEM((devices, 1, size), F32),
            pltpu.VMEM((5, devices, 1, size), F32),
            pltpu.VMEM((devices, 1, size), F32),
            pltpu.VMEM((devices, PEER_TILES, size), F32),
            pltpu.VMEM((devices, PEER_TILES, size), F32),
            pltpu.VMEM((devices, PEER_TILES, size), BF16),
            pltpu.VMEM((devices, PEER_TILES, size), BF16),
            pltpu.VMEM((2, devices, PEER_TILES, size), F32),
            pltpu.VMEM((2, devices, PEER_TILES, size), F32),
            pltpu.VMEM((2, n_col, per_owner, size), F32),
            pltpu.VMEM((2, n_col, per_owner, size), F32),
            pltpu.VMEM((2, per_owner, size), BF16),
            pltpu.VMEM((2, n_col, per_owner, size), BF16),
            pltpu.VMEM((2 * size, rows_dev), BF16),
            pltpu.VMEM((2, devices, gram_rows, size), F32),
            pltpu.VMEM((2, devices, gram_rows, size), F32),
            pltpu.VMEM((2, devices, gram_rows, size), F32),
            pltpu.VMEM((2, per_owner, size), F32),
            pltpu.VMEM((per_owner, size), F32),
            pltpu.VMEM((per_owner, size), F32),
            pltpu.VMEM((size, size), F32),
            pltpu.VMEM((slots, size), BF16),
            pltpu.VMEM((slots, size), F32),
            pltpu.SemaphoreType.DMA((CHUNKS,)),
            pltpu.SemaphoreType.DMA((6,)),
            pltpu.SemaphoreType.DMA((n_phases,)),
            pltpu.SemaphoreType.DMA((n_phases,)),
        ],
        compiler_params=pltpu.CompilerParams(
            collective_id=0, has_side_effects=True, vmem_limit_bytes=60 * 1024 * 1024
        ),
    )(
        tiles, row_tiles.reshape(1, slots), col_tiles.reshape(1, slots), counts, right_basis, left_basis, start.reshape(per_owner, size),
    )
    lefts, rights, line = pl.pallas_call(
        finish,
        out_shape=(
            jax.ShapeDtypeStruct(lefts.shape, F32),
            jax.ShapeDtypeStruct(rights.shape, F32),
            jax.ShapeDtypeStruct((5,), F32),
        ),
        in_specs=[vmem, vmem, pl.BlockSpec(memory_space=pltpu.SMEM)],
        out_specs=(vmem, vmem, pl.BlockSpec(memory_space=pltpu.SMEM)),
    )(lefts, rights, coeffs)
    return lefts, rights, line


def solution(mesh):
    placed = (
        P(("row", "col"), None, None),
        P(("row", "col")),
        P(("row", "col")),
        P(("row", "col")),
        P(None, ("row", "col")),
        P(None, ("row", "col")),
        P(("row", "col")),
    )
    return jax.shard_map(
        shards,
        mesh=mesh,
        in_specs=placed,
        out_specs=(P(None, ("row", "col")), P(None, ("row", "col")), P()),
        check_vma=False,
    )
```

```python
import functools

import jax
import jax.numpy as jnp
from jax import lax
from jax.experimental import pallas as pl
from jax.experimental.pallas import tpu as pltpu
from jax.sharding import PartitionSpec as P

PEER_TILES = 8
GROUP = 16
UNROLL = 16
CHUNKS = 16
DEPTH = 4
EARLY = 4
MESH = pl.DeviceIdType.MESH
F32 = jnp.float32
BF16 = jnp.bfloat16


def hot(condition):
    return jnp.where(condition, 1.0, 0.0).astype(BF16)


def dot(left, right):
    return jnp.dot(left, right, preferred_element_type=F32)


def exact_dot(selector, values):
    high = values.astype(BF16)
    rest = values - high.astype(F32)
    middle = rest.astype(BF16)
    low = (rest - middle.astype(F32)).astype(BF16)
    return dot(selector, high) + (dot(selector, middle) + dot(selector, low))


def kernel(
    n_row, n_col, row_total,
    tiles_hbm, rows_hbm, cols_hbm, counts_hbm, right_hbm, left_hbm, start_hbm,
    lefts_ref, rights_ref, coeffs_ref,
    tiles, flipped, left_ref, right_ref, row_line, col_line, counts_ref, start_ref,
    place_out, place_buf, c_buf, n_buf, pack_first, x_first, pack, xbuf, outgoing, abuf,
    ypart, rsbuf, share, agbuf, halves, gram_out, gram_in, gram_all,
    r_ref, right_one, left_one, acc_ref, x_gathered, products,
    tile_sems, input_sems, send_sems, recv_sems,
):
    devices = n_row * n_col
    my_row = lax.axis_index("row")
    my_col = lax.axis_index("col")
    me = my_row * n_col + my_col
    slots, size = tiles.shape[0], tiles.shape[1]
    per_owner = start_ref.shape[0]
    group_tiles = per_owner * n_col
    table = devices * PEER_TILES
    basis_rows = right_ref.shape[0]
    gram_rows = gram_out.shape[2]

    barrier = pltpu.get_barrier_semaphore()

    if n_col == 4:
        across = lax.rem(my_col + 2, n_col)
        other_cols = [n_col - 1 - my_col, across, n_col - 1 - across]
    else:
        other_cols = [lax.rem(my_col + i, n_col) for i in range(1, n_col)]

    def each_peer(act):
        for col in other_cols:
            def step(i, _, col=col):
                act(lax.rem(my_row + i, n_row), col)
                return 0

            lax.fori_loop(0, n_row, step, 0)

        def own_step(i, _):
            act(lax.rem(my_row + i, n_row), my_col)
            return 0

        lax.fori_loop(1, n_row, own_step, 0)

    each_peer(
        lambda row, col: pl.semaphore_signal(
            barrier, inc=1, device_id={"row": row, "col": col}, device_id_type=MESH
        )
    )

    small = [(start_hbm, start_ref), (rows_hbm, row_line), (cols_hbm, col_line), (counts_hbm, counts_ref)]
    small_copies = [
        pltpu.make_async_copy(source, target, input_sems.at[i])
        for i, (source, target) in enumerate(small)
    ]
    right_copy = pltpu.make_async_copy(right_hbm, right_ref, input_sems.at[len(small)])
    left_copy = pltpu.make_async_copy(left_hbm, left_ref, input_sems.at[len(small) + 1])
    chunk = slots // CHUNKS
    tile_copies = [
        pltpu.make_async_copy(
            tiles_hbm.at[pl.ds(i * chunk, chunk)], tiles.at[pl.ds(i * chunk, chunk)], tile_sems.at[i]
        )
        for i in range(CHUNKS)
    ]
    for copy in [right_copy] + small_copies:
        copy.start()

    phases = [0]

    def next_phase():
        phases[0] += 1
        return phases[0] - 1

    pending = []

    def send_all(source, buf):
        phase = next_phase()

        def send(row, col):
            pltpu.make_async_remote_copy(
                src_ref=source(row * n_col + col), dst_ref=buf.at[me],
                send_sem=send_sems.at[phase], recv_sem=recv_sems.at[phase],
                device_id={"row": row, "col": col}, device_id_type=MESH,
            ).start()

        for col in other_cols:
            for i in range(n_row - 1, -1, -1):
                send(lax.rem(my_row + i, n_row), col)
        for i in range(n_row - 1, 0, -1):
            send(lax.rem(my_row + i, n_row), my_col)
        many = buf.at[pl.ds(0, devices - 1)]
        pending.append((many, phase))
        return lambda: pltpu.make_async_copy(many, many, recv_sems.at[phase]).wait()

    def send_col(source, buf):
        phase = next_phase()
        for col in other_cols:
            pltpu.make_async_remote_copy(
                src_ref=source(col), dst_ref=buf.at[my_col],
                send_sem=send_sems.at[phase], recv_sem=recv_sems.at[phase],
                device_id={"row": my_row, "col": col}, device_id_type=MESH,
            ).start()
        many = buf.at[pl.ds(0, n_col - 1)]
        pending.append((many, phase))
        return lambda: pltpu.make_async_copy(many, many, recv_sems.at[phase]).wait()

    def partial_coeffs(basis, x_ref, buf):
        total = jnp.zeros((basis_rows, size), F32)
        for k in range(per_owner):
            total = total + basis[:, k * size:(k + 1) * size] * x_ref[k:k + 1, :]
        value = x_ref[...]
        acc_ref[0:basis_rows, :] = total
        acc_ref[basis_rows:basis_rows + 1, :] = jnp.sum(value * value, axis=0, keepdims=True)
        buf[me] = jnp.sum(acc_ref[...].T, axis=0, keepdims=True)

    def remainder(basis, x_ref, out_ref, line):
        column = jnp.broadcast_to(line / row_total, (size, size)).T
        for k in range(per_owner):
            part = jnp.sum(
                basis[:, k * size:(k + 1) * size] * column[0:basis_rows, :], axis=0, keepdims=True
            )
            out_ref[k:k + 1, :] = x_ref[k:k + 1, :] - part
        return column

    def gram_norm(line, column, which):
        gram = jnp.concatenate([gram_all[which, i] for i in range(devices)], axis=0)
        weighted = jnp.sum(gram * column, axis=0, keepdims=True)
        lane = lax.broadcasted_iota(jnp.int32, (1, size), 1)
        terms = jnp.where(
            lane < basis_rows,
            line / row_total * (weighted - 2.0 * line),
            jnp.where(lane == basis_rows, line, 0.0),
        )
        total = jnp.maximum(jnp.sum(terms, axis=1, keepdims=True), 0.0)
        return jnp.sqrt(total / row_total + 1e-06)

    def put_coeff(i, value):
        lane = lax.broadcasted_iota(jnp.int32, (1, size), 1)
        line = jnp.broadcast_to(value, (1, size))
        coeffs_ref[...] = line if i == 0 else jnp.where(lane == i, line, coeffs_ref[...])

    def put_rows(ref, row, value):
        for k in range(per_owner):
            ref[row:row + 1, k * size:(k + 1) * size] = value[k:k + 1, :]

    def local_gram(basis, which):
        step = 4 * size

        def split(i, _):
            lanes = pl.ds(pl.multiple_of(i * step, step), step)
            value = basis[:, lanes]
            high = value.astype(BF16)
            halves[0:basis_rows, lanes] = high
            halves[size:size + basis_rows, lanes] = (value - high.astype(F32)).astype(BF16)
            return 0

        lax.fori_loop(0, basis.shape[1] // step, split, 0)
        both = lax.dot_general(
            halves[...], halves[...], (((1,), (1,)), ((), ())), preferred_element_type=F32
        )
        top, bottom = both[0:size, :], both[size:2 * size, :]
        gram = top[:, 0:size] + (
            (top[:, size:2 * size] + bottom[:, 0:size]) + bottom[:, size:2 * size]
        )
        for i in range(devices):
            gram_out[which, i] = gram[i * gram_rows:(i + 1) * gram_rows, :]

    def share_gram_parts(which):
        gram_in[which, me] = gram_out[which, me]
        return send_all(lambda target: gram_out.at[which, target], gram_in.at[which])

    def share_gram_sums(which):
        total = gram_in[which, 0]
        for i in range(1, devices):
            total = total + gram_in[which, i]
        gram_all[which, me] = total
        return send_all(lambda target: gram_all.at[which, me], gram_all.at[which])

    def flip(part):
        tile_copies[part].wait()
        if part + DEPTH < CHUNKS:
            tile_copies[part + DEPTH].start()
        first = part * chunk
        found = [tiles[first + h].T for h in range(chunk)]
        for h in range(chunk):
            flipped[first + h] = found[h]

    acc_ref[...] = jnp.zeros_like(acc_ref)
    for copy in small_copies:
        copy.wait()

    def upright(line):
        return jnp.broadcast_to(line.astype(F32), (size, slots)).T

    live_line = jnp.where(
        lax.broadcasted_iota(jnp.int32, (1, slots), 1) < counts_ref[0], row_line[...], -1
    )
    live_column = upright(live_line)[:, 0:1]
    columns = upright(col_line[...])[:, 0:1].astype(jnp.int32)
    owner = lax.div(columns, per_owner)
    place = lax.rem(columns, per_owner)
    owner_hot = hot(owner == lax.broadcasted_iota(jnp.int32, (slots, devices), 1))
    place_here = place == lax.broadcasted_iota(jnp.int32, (slots, size), 1)
    named = lax.dot_general(
        owner_hot, hot(place_here), (((0,), (0,)), ((), ())), preferred_element_type=F32
    )
    touched = named > 0.5
    earlier = hot(
        lax.broadcasted_iota(jnp.int32, (size, size), 0)
        <= lax.broadcasted_iota(jnp.int32, (size, size), 1)
    )
    rank = jnp.where(touched, dot(hot(touched), earlier) - 1.0, -1.0)
    for i in range(devices):
        place_out[i] = rank[i:i + 1, :]
    place_buf[me] = place_out[me]

    right_copy.wait()
    for copy in [left_copy] + tile_copies[0:DEPTH]:
        copy.start()
    partial_coeffs(right_ref, start_ref, c_buf.at[0])
    pl.semaphore_wait(barrier, devices - 1)
    coeffs_in = send_all(lambda target: c_buf.at[0, me], c_buf.at[0])
    places_in = send_all(lambda target: place_out.at[target], place_buf)

    slot_rank = jnp.sum(
        jnp.where(place_here, dot(owner_hot, rank.astype(BF16)), 0.0), axis=1, keepdims=True
    )
    entry = owner.astype(F32) * PEER_TILES + slot_rank
    entry_hot = hot(entry == lax.broadcasted_iota(jnp.int32, (slots, table), 1).astype(F32))
    entry_line = jnp.broadcast_to(entry, (slots, size)).T[0:1, :]
    entry_hot_t = hot(entry_line == lax.broadcasted_iota(jnp.int32, (table, slots), 0).astype(F32))
    row_hot = hot(
        live_column == lax.broadcasted_iota(jnp.int32, (slots, group_tiles), 1).astype(F32)
    )
    row_hot_t = hot(live_line == lax.broadcasted_iota(jnp.int32, (group_tiles, slots), 0))

    halves[...] = jnp.zeros_like(halves)
    left_copy.wait()
    local_gram(left_ref, 1)
    left_gram_in = share_gram_parts(1)
    for part in range(EARLY):
        flip(part)

    places_in()
    spread = hot(
        lax.div(lax.broadcasted_iota(jnp.int32, (table, devices), 0), PEER_TILES)
        == lax.broadcasted_iota(jnp.int32, (table, devices), 1)
    )
    ranks = jnp.concatenate([place_buf[i] for i in range(devices)], axis=0).astype(BF16)
    wanted = lax.rem(lax.broadcasted_iota(jnp.int32, (table, size), 0), PEER_TILES).astype(F32)
    selector_all = jnp.where(dot(spread, ranks) == wanted, 1.0, 0.0)
    selector = selector_all[:, 0:per_owner].astype(BF16)
    selector_t = selector_all.T[0:per_owner, :].astype(BF16)

    def diagonal(wide):
        index = lax.broadcasted_iota(jnp.int32, (GROUP, size), 0)
        total = wide[:, 0:size]
        for k in range(1, GROUP):
            total = jnp.where(index == k, wide[:, k * size:(k + 1) * size], total)
        return total

    def tile_products(source):
        def one(first):
            vectors = x_gathered[pl.ds(first, GROUP), :]
            block = source[pl.ds(first, GROUP)]
            joined = jnp.concatenate([block[k] for k in range(GROUP)], axis=1)
            return diagonal(dot(vectors, joined))

        def step(g, _):
            firsts = [
                pl.multiple_of(g * (GROUP * UNROLL) + h * GROUP, GROUP) for h in range(UNROLL)
            ]
            found = [one(first) for first in firsts]
            for first, value in zip(firsts, found):
                products[pl.ds(first, GROUP), :] = value
            return 0

        lax.fori_loop(0, slots // (GROUP * UNROLL), step, 0)

    def rows_product(index, values, meanwhile=lambda: None):
        x_gathered[...] = dot(entry_hot, values).astype(BF16)
        tile_products(flipped)
        ypart[index] = exact_dot(row_hot_t, products[...]).reshape(n_col, per_owner, size)
        rows_in = send_col(lambda target: ypart.at[index, target], rsbuf.at[index])
        rsbuf[index, my_col] = ypart[index, my_col]
        meanwhile()
        rows_in()
        total = rsbuf[index, 0]
        for i in range(1, n_col):
            total = total + rsbuf[index, i]
        return total

    def columns_product(index):
        values = agbuf[index].reshape(group_tiles, size)
        x_gathered[...] = dot(row_hot, values).astype(BF16)
        tile_products(tiles)
        outgoing[index] = exact_dot(entry_hot_t, products[...]).reshape(devices, PEER_TILES, size)
        sums_in = send_all(lambda target: outgoing.at[index, target], abuf.at[index])
        abuf[index, me] = outgoing[index, me]
        sums_in()
        return exact_dot(selector_t, abuf[index].reshape(table, size))

    def orthogonalize(basis, which, x_ref, out_ref, index, meanwhile=lambda: None):
        partial_coeffs(basis, x_ref, c_buf.at[index])
        coeffs_in = send_all(lambda target: c_buf.at[index, me], c_buf.at[index])
        meanwhile()
        coeffs_in()
        line = jnp.sum(c_buf[index], axis=0)
        column = remainder(basis, x_ref, out_ref, line)
        norm = gram_norm(line, column, which)
        put_coeff(index, norm)
        return norm, out_ref[...] / norm

    scratch = r_ref
    coeffs_in()
    remainder(right_ref, start_ref, scratch.at[1], jnp.sum(c_buf[0], axis=0))
    value = scratch[1]
    n_buf[me] = jnp.sum(value * value, axis=0, keepdims=True)
    norms_in = send_all(lambda target: n_buf.at[me], n_buf)
    pack_first[...] = exact_dot(selector, value).reshape(devices, PEER_TILES, size)
    values_in = send_all(lambda target: pack_first.at[target], x_first)
    x_first[me] = pack_first[me]
    for part in range(EARLY, CHUNKS):
        flip(part)
    left_gram_in()
    left_gram_in = share_gram_sums(1)
    norms_in()
    norm = jnp.sqrt(
        jnp.sum(jnp.sum(n_buf[...], axis=0), axis=1, keepdims=True) / row_total + 1e-06
    )
    put_coeff(0, norm)
    right_one[...] = scratch[1] / norm
    values_in()

    first_values = (x_first[...].reshape(table, size) / norm).astype(BF16)
    scratch[0] = rows_product(0, first_values, lambda: local_gram(right_ref, 0))
    for index in range(2):
        if index == 0:
            left_gram_in()
        waits = []

        def spread_right_gram():
            if index == 0:
                waits.append(share_gram_parts(0))

        norm, value = orthogonalize(
            left_ref, 1, scratch.at[0], scratch.at[1], 2 * index + 1, spread_right_gram
        )
        share[index] = value.astype(BF16)
        values_in = send_col(lambda target: share.at[index], agbuf.at[index])
        agbuf[index, my_col] = share[index]
        left_one[...] = value
        put_rows(lefts_ref, index, left_one)
        if index == 0:
            waits[0]()
            waits.append(share_gram_sums(0))
        values_in()
        scratch[0] = columns_product(index) - norm * right_one[...]

        if index == 0:
            waits[1]()
        norm, value = orthogonalize(right_ref, 0, scratch.at[0], scratch.at[1], 2 * index + 2)
        if index == 0:
            packed = dot(selector, value.astype(BF16)).reshape(devices, PEER_TILES, size)
            pack[...] = packed.astype(BF16)
            values_in = send_all(lambda target: pack.at[target], xbuf)
            xbuf[me] = pack[me]
        right_one[...] = value
        put_rows(rights_ref, index, right_one)
        if index == 0:
            values_in()
            found = xbuf[...].astype(F32).reshape(table, size).astype(BF16)
            scratch[0] = rows_product(1, found) - norm * left_one[...]

    for many, phase in pending:
        pltpu.make_async_copy(many, many, send_sems.at[phase]).wait()


def finish(lefts_in, rights_in, coeffs_in, lefts, rights, line):
    lefts[...] = lefts_in[...]
    rights[...] = rights_in[...]
    line[...] = coeffs_in[0, 0:line.shape[0]]


def shards(tiles, row_tiles, col_tiles, counts, right_basis, left_basis, start):
    n_row, n_col = lax.axis_size("row"), lax.axis_size("col")
    devices = n_row * n_col
    slots, size = tiles.shape[0], tiles.shape[1]
    rows_dev = start.shape[0]
    per_owner = rows_dev // size
    row_total = float(rows_dev * devices)
    vmem = pl.BlockSpec(memory_space=pltpu.VMEM)
    hbm = pl.BlockSpec(memory_space=pl.ANY)
    n_phases = 19
    gram_rows = size // devices
    lefts, rights, coeffs = pl.pallas_call(
        functools.partial(kernel, n_row, n_col, row_total),
        out_shape=(
            jax.ShapeDtypeStruct((2, rows_dev), F32),
            jax.ShapeDtypeStruct((2, rows_dev), F32),
            jax.ShapeDtypeStruct((1, size), F32),
        ),
        in_specs=[hbm] * 7,
        out_specs=(vmem, vmem, vmem),
        scratch_shapes=[
            pltpu.VMEM(tiles.shape, BF16),
            pltpu.VMEM(tiles.shape, BF16),
            pltpu.VMEM(left_basis.shape, F32),
            pltpu.VMEM(right_basis.shape, F32),
            pltpu.VMEM((1, slots), jnp.int32),
            pltpu.VMEM((1, slots), jnp.int32),
            pltpu.SMEM((1,), jnp.int32),
            pltpu.VMEM((per_owner, size), F32),
            pltpu.VMEM((devices, 1, size), F32),
            pltpu.VMEM((devices, 1, size), F32),
            pltpu.VMEM((5, devices, 1, size), F32),
            pltpu.VMEM((devices, 1, size), F32),
            pltpu.VMEM((devices, PEER_TILES, size), F32),
            pltpu.VMEM((devices, PEER_TILES, size), F32),
            pltpu.VMEM((devices, PEER_TILES, size), BF16),
            pltpu.VMEM((devices, PEER_TILES, size), BF16),
            pltpu.VMEM((2, devices, PEER_TILES, size), F32),
            pltpu.VMEM((2, devices, PEER_TILES, size), F32),
            pltpu.VMEM((2, n_col, per_owner, size), F32),
            pltpu.VMEM((2, n_col, per_owner, size), F32),
            pltpu.VMEM((2, per_owner, size), BF16),
            pltpu.VMEM((2, n_col, per_owner, size), BF16),
            pltpu.VMEM((2 * size, rows_dev), BF16),
            pltpu.VMEM((2, devices, gram_rows, size), F32),
            pltpu.VMEM((2, devices, gram_rows, size), F32),
            pltpu.VMEM((2, devices, gram_rows, size), F32),
            pltpu.VMEM((2, per_owner, size), F32),
            pltpu.VMEM((per_owner, size), F32),
            pltpu.VMEM((per_owner, size), F32),
            pltpu.VMEM((size, size), F32),
            pltpu.VMEM((slots, size), BF16),
            pltpu.VMEM((slots, size), F32),
            pltpu.SemaphoreType.DMA((CHUNKS,)),
            pltpu.SemaphoreType.DMA((6,)),
            pltpu.SemaphoreType.DMA((n_phases,)),
            pltpu.SemaphoreType.DMA((n_phases,)),
        ],
        compiler_params=pltpu.CompilerParams(
            collective_id=0, has_side_effects=True, vmem_limit_bytes=60 * 1024 * 1024
        ),
    )(
        tiles, row_tiles.reshape(1, slots), col_tiles.reshape(1, slots), counts, right_basis, left_basis, start.reshape(per_owner, size),
    )
    lefts, rights, line = pl.pallas_call(
        finish,
        out_shape=(
            jax.ShapeDtypeStruct(lefts.shape, F32),
            jax.ShapeDtypeStruct(rights.shape, F32),
            jax.ShapeDtypeStruct((5,), F32),
        ),
        in_specs=[vmem] * 3,
        out_specs=(vmem,) * 3,
    )(lefts, rights, coeffs)
    return lefts, rights, line


def solution(mesh):
    placed = (
        P(("row", "col"), None, None),
        P(("row", "col")),
        P(("row", "col")),
        P(("row", "col")),
        P(None, ("row", "col")),
        P(None, ("row", "col")),
        P(("row", "col")),
    )
    return jax.shard_map(
        shards,
        mesh=mesh,
        in_specs=placed,
        out_specs=(P(None, ("row", "col")), P(None, ("row", "col")), P()),
        check_vma=False,
    )
```
